512 devices in a mesh: seq: 32 (over y, z_hi), section: 4 (over x), tp: 4 (over z_lo, core).
Axes of the slice: x: 4, y: 8, z: 8 (z_hi: 4, z_lo: 2; z = z_hi * 2 + z_lo), core: 2. Of those that a mesh axis runs over, the one named last changes fastest.
Arguments:
- token_ids: int32 [2048], P('seq'), may hold values from 0 to 65535
- embed_columns: bfloat16 [4096, 65536], P(('tp', 'seq')), may hold values from -6 to 6
- norm_gain: bfloat16 [4, 4096], P('section'), may hold values from 0.099609375 to 1.8984375
- qkv_weight: bfloat16 [4, 4096, 4096], P('section', 'seq', 'tp'), may hold values from -1 to 1
- out_weight: bfloat16 [4, 4096, 2048], P('section', 'seq', 'tp'), may hold values from -0.125 to 0.125
Outputs:
- layer_states: bfloat16 [4, 2048, 4096], P('section', 'seq', 'tp')
The draws below stay inside these ranges and needn't reach their ends.
All inputs are finite; a program needn't handle non-finite values.
Results may differ from the reference program's by a relative error of at most 0.02.
Values may be sent and summed in bfloat16 or wider, within the bound.
A program may use at most 128 MiB of HBM per device.

```python
import math
import jax
import jax.numpy as jnp
import numpy as np
from jax import lax

D = 4096
QUERY_HEADS = 16
KEY_VALUE_HEADS = 8
HEAD_WIDTH = 128
VOCAB = 65536
BLOCK = 64
LAYERS = 4
CONTEXT_TOKENS = 2048
N_SEQ = 32
N_TP = 4


def draw_qkv_weight(key, part):
    group_factor = N_TP
    query_heads = QUERY_HEADS // group_factor
    key_value_heads = KEY_VALUE_HEADS // group_factor
    drawn = jax.random.normal(key, (LAYERS, D, group_factor, query_heads + 2 * key_value_heads, HEAD_WIDTH), jnp.float32) * D ** (-0.5)
    drawn = jnp.clip(drawn, -1.0, 1.0)
    return drawn.reshape(LAYERS, D, group_factor * (query_heads + 2 * key_value_heads) * HEAD_WIDTH).astype(jnp.bfloat16)


def plant(values, key, least, top_value):
    index_at = [jax.random.randint(jax.random.fold_in(key, axis), (), 0, length) for axis, length in enumerate(values.shape)]
    widest = values.shape.index(max(values.shape))
    next_to = index_at[:widest] + [(index_at[widest] + 1) % values.shape[widest]] + index_at[widest + 1:]
    return values.at[tuple(index_at)].set(least).at[tuple(next_to)].set(top_value)


def level_of(stream_key, dims, split, low, top_value):
    loudness, own = 1.0, jax.random.fold_in(stream_key, 6)
    for dim, blocks in split:
        draws = jnp.exp(jax.random.uniform(jax.random.fold_in(own, dim), (blocks,), jnp.float32, low / len(split), top_value / len(split)))
        loudness = loudness * jnp.repeat(draws, dims[dim] // blocks).reshape([-1 if axis == dim else 1 for axis in range(len(dims))])
    return loudness


def cumulative_ranks(count, lean):
    portions = [(1 << 20) // math.isqrt(standing ** lean) + 1 for standing in range(1, count + 1)]
    scale = 1 + sum(portions) // (1 << 30)
    return np.cumsum(np.array([max(1, weight // scale) for weight in portions]))


def skewed_ids(own_key, extent, amount, lean):
    grid = cumulative_ranks(amount, lean)
    pick = jax.random.randint(jax.random.fold_in(own_key, 1), extent, 0, int(grid[amount - 1]))
    grade = jnp.searchsorted(jnp.asarray(grid, jnp.int32), pick, side="right")
    return jax.random.permutation(jax.random.fold_in(own_key, 2), amount)[grade].astype(jnp.int32)


def bell_draw(stream_key, shape, scale, limit, pieces=(), kind=jnp.bfloat16):
    array = scale * jax.random.normal(stream_key, shape, jnp.float32)
    if pieces:
        array = array * level_of(stream_key, shape, pieces, -0.22, 0.18)
    return jnp.clip(array, -limit, limit).astype(kind)


def setup_inputs(seed: int = 0) -> dict:
    splits = jax.random.split(jax.random.key(seed), 6)
    return {
        "token_ids": plant(skewed_ids(splits[0], (CONTEXT_TOKENS,), VOCAB, 2), jax.random.fold_in(splits[0], 3), 0, VOCAB - 1).astype(jnp.int32),
        "embed_columns": bell_draw(splits[1], (D, VOCAB), 1.0, 6.0, ((0, 128),)),
        "norm_gain": jnp.clip(1.0 + 0.18 * jax.random.normal(splits[2], (LAYERS, D), jnp.float32), 0.099609375, 1.8984375).astype(jnp.bfloat16),
        "qkv_weight": draw_qkv_weight(jax.random.fold_in(splits[5], 71), 0),
        "out_weight": bell_draw(splits[4], (LAYERS, D, QUERY_HEADS * HEAD_WIDTH), (QUERY_HEADS * HEAD_WIDTH) ** -0.5, 0.125, ((0, 4), (1, 32), (2, 4))),
    }


EPS = 1e-05
ROPE_BASE = 500000.0
MASKED = -1e+30

def rope_tables(positions, head_size):
    half_width = head_size // 2
    inverse_freq = ROPE_BASE ** (-jnp.arange(half_width).astype(jnp.float32) * (2.0 / head_size))
    angles = positions.astype(jnp.float32)[:, None] * inverse_freq[None, :]
    return (jnp.cos(angles), jnp.sin(angles))

def rotate_half(heads, cosine_table, sine_values):
    half_width = heads.shape[-1] // 2
    first_half = heads[..., :half_width]
    second = heads[..., half_width:]
    cosine_table = cosine_table[:, None, :]
    sine_values = sine_values[:, None, :]
    return jnp.concatenate([first_half * cosine_table - second * sine_values, second * cosine_table + first_half * sine_values], axis=-1)

def norm_rows(row_block, gain_row):
    values = row_block.astype(jnp.float32)
    inverse_rms = lax.rsqrt(lax.optimization_barrier(jnp.mean(values * values, axis=-1, keepdims=True)) + EPS)
    return (values * inverse_rms * gain_row.astype(jnp.float32)[None, :]).astype(jnp.bfloat16)

def reference(token_ids, embed_columns, norm_gain, qkv_weight, out_weight):
    group_factor = N_SEQ
    block_row_slice = BLOCK
    query_heads = QUERY_HEADS // N_TP
    key_value_heads = KEY_VALUE_HEADS // N_TP
    repeat_heads = QUERY_HEADS // KEY_VALUE_HEADS
    hidden = jnp.take(embed_columns, token_ids, axis=1).T
    positions = jnp.arange(CONTEXT_TOKENS).astype(jnp.int32)
    cosine_table, sine_values = rope_tables(positions, HEAD_WIDTH)
    row_ids = jnp.arange(block_row_slice)[None, :, None]
    column = jnp.arange(2 * block_row_slice)[None, None, :]
    group_ids = jnp.arange(group_factor)[:, None, None]
    allowed = jnp.where(column < block_row_slice, group_ids > 0, column - block_row_slice <= row_ids)
    states = []
    for layer_index in range(LAYERS):
        normed = norm_rows(hidden, norm_gain[layer_index])
        projected_rows = jnp.dot(normed, qkv_weight[layer_index], preferred_element_type=jnp.float32)
        projected_rows = projected_rows.reshape(CONTEXT_TOKENS, N_TP, query_heads + 2 * key_value_heads, HEAD_WIDTH)
        query_rows = rotate_half(projected_rows[:, :, :query_heads].reshape(CONTEXT_TOKENS, QUERY_HEADS, HEAD_WIDTH), cosine_table, sine_values).astype(jnp.bfloat16)
        key_head_rows = rotate_half(projected_rows[:, :, query_heads:query_heads + key_value_heads].reshape(CONTEXT_TOKENS, KEY_VALUE_HEADS, HEAD_WIDTH), cosine_table, sine_values).astype(jnp.bfloat16)
        value_head_rows = projected_rows[:, :, query_heads + key_value_heads:].reshape(CONTEXT_TOKENS, KEY_VALUE_HEADS, HEAD_WIDTH).astype(jnp.bfloat16)
        key_head_rows = key_head_rows.reshape(group_factor, block_row_slice, KEY_VALUE_HEADS, HEAD_WIDTH)
        value_head_rows = value_head_rows.reshape(group_factor, block_row_slice, KEY_VALUE_HEADS, HEAD_WIDTH)
        both_keys = jnp.concatenate([jnp.broadcast_to(key_head_rows[:1], key_head_rows.shape), key_head_rows], axis=1)
        both_values = jnp.concatenate([jnp.broadcast_to(value_head_rows[:1], value_head_rows.shape), value_head_rows], axis=1)
        query_groups = query_rows.reshape(group_factor, block_row_slice, KEY_VALUE_HEADS, repeat_heads, HEAD_WIDTH).astype(jnp.float32)
        scores = jnp.einsum('grkph,gckh->gkprc', query_groups, both_keys.astype(jnp.float32)) * HEAD_WIDTH ** (-0.5)
        scores = jnp.where(allowed[:, None, None], scores, MASKED)
        weights = jax.nn.softmax(scores, axis=-1).astype(jnp.bfloat16)
        attended = jnp.einsum('gkprc,gckh->grkph', weights.astype(jnp.float32), both_values.astype(jnp.float32)).astype(jnp.bfloat16)
        attended = attended.reshape(CONTEXT_TOKENS, N_TP, query_heads * HEAD_WIDTH)
        out_heads = out_weight[layer_index].reshape(D, N_TP, query_heads * HEAD_WIDTH)
        partial_value = jnp.einsum('rtc,dtc->trd', attended.astype(jnp.float32), out_heads.astype(jnp.float32)).astype(jnp.bfloat16)
        partial_value = lax.optimization_barrier(partial_value)
        summed = lax.optimization_barrier(jnp.sum(partial_value.astype(jnp.float32), axis=0))
        hidden = (hidden.astype(jnp.float32) + summed).astype(jnp.bfloat16)
        states.append(hidden)
    return jnp.stack(states)
```

```python
import functools

import jax
import jax.numpy as jnp
import numpy as np
from jax import lax
from jax.experimental import pallas as pl
from jax.experimental.pallas import tpu as pltpu
from jax.sharding import PartitionSpec as P

MESH = pl.DeviceIdType.MESH
LAYERS = 4
NY = 8
NZ = 4
SEQ = NY * NZ
GROUP = 8
ROWS = 128
BLOCK = 64
HEAD = 128
WIDE = 768
SLICE = 512
EPS = 1e-05
ROPE_BASE = 500000.0
MASKED = -1e30
Z_STEPS = (0, 1, 3, 2)


def remote(src, dst, send, recv, seq, section, tp):
    return pltpu.make_async_remote_copy(
        src_ref=src,
        dst_ref=dst,
        send_sem=send,
        recv_sem=recv,
        device_id=(seq, section, tp),
        device_id_type=MESH,
    )


def kernel(
    ids_ref, table_ref, wsrc_ref, rope_a_ref, rope_b_ref, out_ref,
    w, tab, ids_v, ids_s, emb_out, emb_in, hid, part_out, part_in, kv, akv, acc, res,
    x_send, x_recv, z_send, z_recv, y_send, y_recv, push_send, push_recv,
    ids_send, ids_recv, ids_local, tab_sem, emb_send, emb_recv,
    ag_send, ag_recv, rs_send, rs_recv, kv_send, kv_recv, out_send, out_recv,
):
    seq = lax.axis_index("seq")
    x = lax.axis_index("section")
    tp = lax.axis_index("tp")
    y = seq // NZ
    zh = seq % NZ
    zl = tp // 2
    c = tp % 2
    m = 4 * zl + x
    comm = 2 * zl
    chain = 2 * zl + 1
    is_comm = c == 0
    is_chain = c == 1

    def x_copy(j):
        return remote(
            wsrc_ref.at[j], w.at[x, seq], x_send.at[j], x_recv.at[x], seq, 2 * c + j, comm
        )

    for j in range(2):
        stays = is_comm & (x == j)

        @pl.when(jnp.logical_not(stays))
        def _():
            x_copy(j).start()

        @pl.when(stays)
        def _():
            w[x, seq] = wsrc_ref[j]

    @pl.loop(0, tab.shape[0])
    def _(k):
        columns = pl.ds(pl.multiple_of(k * HEAD, HEAD), HEAD)
        pltpu.make_async_copy(table_ref.at[:, columns], tab.at[k], tab_sem).start()

    def ids_copy(d):
        return remote(
            ids_ref, ids_v.at[y], ids_send.at[d], ids_recv.at[y], (seq + d) % SEQ, x, tp
        )

    @pl.when(zh == x)
    def _():
        @pl.loop(1, SEQ)
        def _(d):
            ids_copy(d).start()

        ids_v[y] = ids_ref[...]

    def z_copy(layer, dz):
        return remote(
            w.at[layer, seq], w.at[layer, seq], z_send.at[layer], z_recv.at[layer, dz],
            NZ * y + (zh + dz) % NZ, x, comm,
        )

    def push(layer, s):
        remote(
            w.at[layer, s], w.at[layer, s], push_send.at[layer], push_recv.at[layer], seq, x, chain
        ).start()

    def y_copy(layer, way, step, zi, s):
        to = (seq + (NZ if way == 0 else SEQ - NZ)) % SEQ
        return remote(
            w.at[layer, s], w.at[layer, s], y_send.at[layer, way], y_recv.at[layer, way, step, zi],
            to, x, comm,
        )

    @pl.when(is_comm)
    def _():
        for layer in range(LAYERS):
            local = (x == layer) & (x < 2)

            @pl.when(jnp.logical_not(local))
            def _():
                remote(
                    w.at[layer, seq], w.at[layer, seq], x_send.at[0], x_recv.at[layer], seq, x, comm
                ).wait_recv()

            for dz in (1, 3, 2):
                z_copy(layer, dz).start()
            if layer == 0:
                for way in range(2):
                    y_copy(0, way, 0, 0, seq).start()
            push(layer, seq)

    @pl.loop(0, NY)
    def _(b):
        @pl.when(jnp.logical_not((zh == x) & (b == y)))
        def _():
            remote(
                ids_ref, ids_v.at[b], ids_send.at[0], ids_recv.at[b], seq, x, tp
            ).wait_recv()

    to_scalar = pltpu.make_async_copy(ids_v, ids_s, ids_local)
    to_scalar.start()
    to_scalar.wait()
    pltpu.make_async_copy(tab, tab, tab_sem).wait()
    emb_section = 2 * c + seq // 16
    lane = lax.broadcasted_iota(jnp.int32, (32, HEAD), 1)

    def emb_copy(b):
        return remote(
            emb_out.at[b], emb_in.at[seq % 16], emb_send.at[b], emb_recv.at[seq % 16],
            NZ * b + x, emb_section, chain,
        )

    def emb_self(b):
        return is_chain & (emb_section == x) & (NZ * b + x == seq)

    @pl.loop(0, NY)
    def _(b):
        def token(i, got):
            v = ids_s[b, 0, i]
            tile = tab[v >> 7].astype(jnp.float32)
            column = jnp.sum(jnp.where(lane == (v & 127), tile, 0.0), axis=1, keepdims=True)
            return jnp.where(lane == i, column, got)

        got = lax.fori_loop(0, BLOCK, token, jnp.zeros((32, HEAD), jnp.float32), unroll=8)
        emb_out[b] = got.astype(jnp.bfloat16)

        @pl.when(jnp.logical_not(emb_self(b)))
        def _():
            emb_copy(b).start()

        @pl.when(emb_self(b))
        def _():
            emb_in[seq % 16] = got.astype(jnp.bfloat16)

    def own_sends(layer, first):
        for zi in range(first, NZ):
            dz = Z_STEPS[zi]
            s = NZ * y + (zh + NZ - dz) % NZ
            if zi > 0:
                remote(
                    w.at[layer, s], w.at[layer, s], z_send.at[layer], z_recv.at[layer, dz],
                    seq, x, comm,
                ).wait_recv()
            for way in range(2):
                y_copy(layer, way, 0, zi, s).start()
            if zi > 0:
                push(layer, s)

    def received(way, step, zi):
        row = (y + (NY - step if way == 0 else step)) % NY
        return NZ * row + (zh + NZ - Z_STEPS[zi]) % NZ

    def arrived(layer, way, step, zi):
        s = received(way, step, zi)
        y_copy(layer, way, step - 1, zi, s).wait_recv()
        return s

    @pl.when(is_comm)
    def _():
        own_sends(0, 1)

        @pl.loop(0, LAYERS)
        def _(layer):
            for step in range(1, 4):
                for zi in range(NZ):
                    for way in range(2):
                        s = arrived(layer, way, step, zi)
                        if step < 3 or (zi < 2) == (way == 0):
                            y_copy(layer, way, step, zi, s).start()
                        push(layer, s)

            @pl.when(layer < LAYERS - 1)
            def _():
                own_sends(layer + 1, 0)

            for zi in range(NZ):
                push(layer, arrived(layer, 0 if zi < 2 else 1, 4, zi))

        @pl.loop(0, LAYERS)
        def _(layer):
            for way in range(2):
                remote(
                    w.at[layer, pl.ds(0, 14)], w.at[layer, pl.ds(0, 14)], y_send.at[layer, way],
                    y_recv.at[layer, way, 0, 0], seq, x, comm,
                ).wait_send()
            remote(
                w.at[layer, pl.ds(0, 3)], w.at[layer, pl.ds(0, 3)], z_send.at[layer],
                z_recv.at[layer, 1], seq, x, comm,
            ).wait_send()
            remote(
                w.at[layer], w.at[layer], push_send.at[layer], push_recv.at[layer], seq, x, chain
            ).wait_send()

    def member(d):
        other = m ^ d
        return other, other % 4, 2 * (other // 4) + 1

    def ag_copy(layer, d):
        _, section, to = member(d)
        return remote(
            hid.at[layer, m], hid.at[layer, m], ag_send.at[layer], ag_recv.at[layer, m],
            seq, section, to,
        )

    def rs_copy(layer, d):
        other, section, to = member(d)
        return remote(
            part_out.at[layer, other], part_in.at[layer, m], rs_send.at[layer],
            rs_recv.at[layer, m], seq, section, to,
        )

    def kv_copy(layer, src, i, to):
        return remote(src, akv.at[layer], kv_send.at[layer, i], kv_recv.at[layer], to, x, tp)

    def out_copy(layer):
        return remote(
            hid.at[layer + 1, m], out_ref.at[:, pl.ds(pl.multiple_of((x % 2) * SLICE, SLICE), SLICE)],
            out_send.at[layer], out_recv.at[x % 2], seq, layer, 2 * zl + x // 2,
        )

    def out_self(layer):
        return (layer == x) & (x >= 2)

    @pl.when(is_chain)
    def _():
        self_emb = (zh == x) & (x >= 2) & (seq // 16 == x % 2)

        @pl.loop(0, 16)
        def _(k):
            @pl.when(jnp.logical_not(self_emb & (k == seq % 16)))
            def _():
                remote(
                    emb_out.at[0], emb_in.at[k], emb_send.at[0], emb_recv.at[k], seq, x, tp
                ).wait_recv()

        start = emb_in[...].reshape(SLICE, HEAD).astype(jnp.float32).T[:BLOCK]
        res[...] = start
        hid[0, m] = start.astype(jnp.bfloat16)
        for d in range(1, GROUP):
            ag_copy(0, d).start()

        a = rope_a_ref[pl.ds(seq, 1), :]
        cos_a, sin_a = a[:, :HEAD], a[:, HEAD:]
        cos_b, sin_b = rope_b_ref[:, :HEAD], rope_b_ref[:, HEAD:]
        cosine = cos_a * cos_b - sin_a * sin_b
        sine = sin_a * cos_b + cos_a * sin_b
        side = lax.broadcasted_iota(jnp.int32, (BLOCK, HEAD), 1)
        sine = jnp.where(side < HEAD // 2, -sine, sine)

        def rotated(v):
            return (v * cosine + pltpu.roll(v, HEAD // 2, 1) * sine).astype(jnp.bfloat16)

        row = lax.broadcasted_iota(jnp.int32, (2 * BLOCK, 2 * BLOCK), 0) % BLOCK
        col = lax.broadcasted_iota(jnp.int32, (2 * BLOCK, 2 * BLOCK), 1)
        allowed = ((col < BLOCK) & (seq > 0)) | ((col >= BLOCK) & (col - BLOCK <= row))

        @pl.loop(0, LAYERS)
        def _(layer):
            remote(
                w.at[layer], w.at[layer], push_send.at[layer], push_recv.at[layer], seq, x, chain
            ).wait_recv()

            def add(d, square):
                other = m ^ d

                @pl.when(d > 0)
                def _():
                    remote(
                        hid.at[layer, other], hid.at[layer, other], ag_send.at[layer],
                        ag_recv.at[layer, other], seq, x, chain,
                    ).wait_recv()

                h = hid[layer, other]
                weights = w[layer, pl.ds(4 * other, 4), :, :SLICE].reshape(SLICE, SLICE)
                product = jnp.dot(h, weights, preferred_element_type=jnp.float32)

                @pl.when(d == 0)
                def _():
                    acc[...] = product

                @pl.when(d > 0)
                def _():
                    acc[...] += product

                hf = h.astype(jnp.float32)
                return square + jnp.sum(hf * hf, axis=1, keepdims=True)

            square = lax.fori_loop(0, GROUP, add, jnp.zeros((BLOCK, 1), jnp.float32))
            projected = acc[...] * lax.rsqrt(square * (1.0 / (GROUP * SLICE)) + EPS)
            q0 = rotated(projected[:, :HEAD])
            q1 = rotated(projected[:, HEAD : 2 * HEAD])
            key = rotated(projected[:, 2 * HEAD : 3 * HEAD])
            value = projected[:, 3 * HEAD :].astype(jnp.bfloat16)
            kv[layer, :, :HEAD] = key
            kv[layer, :, HEAD:] = value

            @pl.when(seq == 0)
            def _():
                for i in range(1, NY):
                    kv_copy(layer, kv.at[layer], i, NZ * i).start()
                for i in range(1, NZ):
                    kv_copy(layer, kv.at[layer], NY + i, i).start()
                akv[layer, :, :HEAD] = key
                akv[layer, :, HEAD:] = value

            @pl.when(seq > 0)
            def _():
                kv_copy(layer, kv.at[layer], 0, seq).wait_recv()

                @pl.when(zh == 0)
                def _():
                    for i in range(1, NZ):
                        kv_copy(layer, akv.at[layer], NY + i, seq + i).start()

            queries = jnp.concatenate([q0, q1], axis=0)
            keys = jnp.concatenate([akv[layer, :, :HEAD], key], axis=0)
            values = jnp.concatenate([akv[layer, :, HEAD:], value], axis=0)
            scores = lax.dot_general(
                queries, keys, (((1,), (1,)), ((), ())), preferred_element_type=jnp.float32
            ) * (HEAD ** -0.5)
            scores = jnp.where(allowed, scores, MASKED)
            e = jnp.exp(scores - jnp.max(scores, axis=1, keepdims=True))
            probs = (e / jnp.sum(e, axis=1, keepdims=True)).astype(jnp.bfloat16)
            both = jnp.dot(probs, values, preferred_element_type=jnp.float32).astype(jnp.bfloat16)
            attended = jnp.concatenate([both[:BLOCK], both[BLOCK:]], axis=1)

            def partial(other):
                weights = w[layer, pl.ds(4 * other, 4), :, SLICE:].reshape(SLICE, 2 * HEAD)
                return lax.dot_general(
                    attended, weights, (((1,), (1,)), ((), ())), preferred_element_type=jnp.float32
                )

            @pl.loop(1, GROUP)
            def _(d):
                other = m ^ d
                part_out[layer, other] = partial(other).astype(jnp.bfloat16)
                rs_copy(layer, d).start()

            acc[...] = partial(m)

            @pl.loop(1, GROUP)
            def _(d):
                other = m ^ d
                remote(
                    part_out.at[layer, other], part_in.at[layer, other], rs_send.at[layer],
                    rs_recv.at[layer, other], seq, x, chain,
                ).wait_recv()
                acc[...] += part_in[layer, other].astype(jnp.float32)

            new = (res[...] + acc[...]).astype(jnp.bfloat16)
            res[...] = new.astype(jnp.float32)
            hid[layer + 1, m] = new

            @pl.when(layer < LAYERS - 1)
            def _():
                for d in range(1, GROUP):
                    ag_copy(layer + 1, d).start()

            @pl.when(jnp.logical_not(out_self(layer)))
            def _():
                out_copy(layer).start()

            @pl.when(out_self(layer))
            def _():
                out_ref[:, pl.ds(pl.multiple_of((x % 2) * SLICE, SLICE), SLICE)] = new

        @pl.loop(0, LAYERS)
        def _(layer):
            remote(
                hid.at[layer, pl.ds(0, 7)], hid.at[layer, pl.ds(0, 7)], ag_send.at[layer],
                ag_recv.at[layer, 0], seq, x, chain,
            ).wait_send()
            remote(
                part_out.at[layer, pl.ds(0, 7)], part_in.at[layer, pl.ds(0, 7)], rs_send.at[layer],
                rs_recv.at[layer, 0], seq, x, chain,
            ).wait_send()

            @pl.when(seq == 0)
            def _():
                for i in range(1, NY):
                    kv_copy(layer, kv.at[layer], i, seq).wait_send()

            @pl.when(zh == 0)
            def _():
                for i in range(1, NZ):
                    kv_copy(layer, kv.at[layer], NY + i, seq).wait_send()

            @pl.when(jnp.logical_not(out_self(layer)))
            def _():
                out_copy(layer).wait_send()

    for j in range(2):
        @pl.when(jnp.logical_not(is_comm & (x == j)))
        def _():
            x_copy(j).wait_send()

    @pl.when(zh == x)
    def _():
        @pl.loop(1, SEQ)
        def _(d):
            ids_copy(d).wait_send()

    @pl.loop(0, NY)
    def _(b):
        @pl.when(jnp.logical_not(emb_self(b)))
        def _():
            emb_copy(b).wait_send()

    for half in range(2):
        @pl.when(jnp.logical_not(is_chain & (x == 2 + half)))
        def _():
            remote(
                hid.at[0, 0], out_ref.at[:, pl.ds(half * SLICE, SLICE)], out_send.at[0],
                out_recv.at[half], seq, x, tp,
            ).wait_recv()


def rope_constants():
    half = np.arange(HEAD // 2, dtype=np.float64)
    freq = np.float64(ROPE_BASE) ** (-2.0 * half / HEAD)
    freq = np.concatenate([freq, freq])
    coarse = np.arange(SEQ, dtype=np.float64)[:, None] * BLOCK * freq[None]
    fine = np.arange(BLOCK, dtype=np.float64)[:, None] * freq[None]
    pair = lambda angle: np.concatenate([np.cos(angle), np.sin(angle)], axis=1).astype(np.float32)
    return pair(coarse), pair(fine)


def body(token_ids, embed_columns, norm_gain, qkv_weight, out_weight):
    seq = lax.axis_index("seq")
    ids = jnp.broadcast_to(jnp.pad(token_ids, (0, HEAD - BLOCK))[None], (8, HEAD))
    gain = lax.dynamic_slice_in_dim(norm_gain[0], seq * ROWS, ROWS, 0).astype(jnp.float32)
    qkv = (qkv_weight[0].astype(jnp.float32) * gain[:, None]).astype(jnp.bfloat16)
    out = out_weight[0]
    pieces = [
        jnp.concatenate(
            [
                qkv[:, 2 * HEAD * j : 2 * HEAD * (j + 1)],
                qkv[:, HEAD * (4 + j) : HEAD * (5 + j)],
                qkv[:, HEAD * (6 + j) : HEAD * (7 + j)],
                out[:, 2 * HEAD * j : 2 * HEAD * (j + 1)],
            ],
            axis=1,
        )
        for j in range(2)
    ]
    sources = jnp.stack(pieces)
    rope_a, rope_b = rope_constants()
    bf16, f32 = jnp.bfloat16, jnp.float32
    vmem = pl.BlockSpec(memory_space=pltpu.VMEM)
    dma = pltpu.SemaphoreType.DMA
    states = pl.pallas_call(
        kernel,
        out_shape=jax.ShapeDtypeStruct((BLOCK, 2 * SLICE), bf16),
        in_specs=[vmem, pl.BlockSpec(memory_space=pl.ANY), vmem, vmem, vmem],
        out_specs=vmem,
        scratch_shapes=[
            pltpu.VMEM((LAYERS, SEQ, ROWS, WIDE), bf16),
            pltpu.VMEM((embed_columns.shape[1] // HEAD, 32, HEAD), bf16),
            pltpu.VMEM((NY, 8, HEAD), jnp.int32),
            pltpu.SMEM((NY, 8, HEAD), jnp.int32),
            pltpu.VMEM((NY, 32, HEAD), bf16),
            pltpu.VMEM((16, 32, HEAD), bf16),
            pltpu.VMEM((LAYERS + 1, GROUP, BLOCK, SLICE), bf16),
            pltpu.VMEM((LAYERS, GROUP, BLOCK, SLICE), bf16),
            pltpu.VMEM((LAYERS, GROUP, BLOCK, SLICE), bf16),
            pltpu.VMEM((LAYERS, BLOCK, 2 * HEAD), bf16),
            pltpu.VMEM((LAYERS, BLOCK, 2 * HEAD), bf16),
            pltpu.VMEM((BLOCK, SLICE), f32),
            pltpu.VMEM((BLOCK, SLICE), f32),
            dma((2,)),
            dma((LAYERS,)),
            dma((LAYERS,)),
            dma((LAYERS, NZ)),
            dma((LAYERS, 2)),
            dma((LAYERS, 2, 4, NZ)),
            dma((LAYERS,)),
            dma((LAYERS,)),
            dma((SEQ,)),
            dma((NY,)),
            dma,
            dma,
            dma((NY,)),
            dma((16,)),
            dma((LAYERS,)),
            dma((LAYERS, GROUP)),
            dma((LAYERS,)),
            dma((LAYERS, GROUP)),
            dma((LAYERS, NY + NZ)),
            dma((LAYERS,)),
            dma((LAYERS,)),
            dma((2,)),
        ],
        compiler_params=pltpu.CompilerParams(
            has_side_effects=True, vmem_limit_bytes=62 * 1024 * 1024
        ),
    )(ids, embed_columns, sources, jnp.asarray(rope_a), jnp.asarray(rope_b))
    return states[None]


def solution(mesh):
    placed = (
        P("seq"),
        P(("tp", "seq"), None),
        P("section", None),
        P("section", "seq", "tp"),
        P("section", "seq", "tp"),
    )
    return jax.shard_map(
        body, mesh=mesh, in_specs=placed, out_specs=P("section", "seq", "tp"), check_vma=False
    )
```

```python
import functools

import jax
import jax.numpy as jnp
import numpy as np
from jax import lax
from jax.experimental import pallas as pl
from jax.experimental.pallas import tpu as pltpu
from jax.sharding import PartitionSpec as P

MESH = pl.DeviceIdType.MESH
LAYERS = 4
NY = 8
NZ = 4
SEQ = NY * NZ
GROUP = 8
ROWS = 128
BLOCK = 64
HEAD = 128
WIDE = 768
SLICE = 512
EPS = 1e-05
ROPE_BASE = 500000.0
MASKED = -1e30
Z_STEPS = (0, 1, 3, 2)


def remote(src, dst, send, recv, seq, section, tp):
    return pltpu.make_async_remote_copy(
        src_ref=src,
        dst_ref=dst,
        send_sem=send,
        recv_sem=recv,
        device_id=(seq, section, tp),
        device_id_type=MESH,
    )


def kernel(
    token_ref, table_ref, gain_ref, qkv_ref, proj_ref, rope_a_ref, rope_b_ref, out_ref,
    ids_ref, wsrc_ref, w, tab, ids_v, ids_s, emb_out, emb_in, hid, part_out, part_in, kv, akv, acc, res,
    x_send, x_recv, z_send, z_recv, y_send, y_recv, push_send, push_recv,
    ids_send, ids_recv, ids_local, tab_sem, emb_send, emb_recv,
    ag_send, ag_recv, rs_send, rs_recv, kv_send, kv_recv, out_send, out_recv,
):
    seq = lax.axis_index("seq")
    x = lax.axis_index("section")
    tp = lax.axis_index("tp")
    y = seq // NZ
    zh = seq % NZ
    zl = tp // 2
    c = tp % 2
    m = 4 * zl + x
    comm = 2 * zl
    chain = 2 * zl + 1
    is_comm = c == 0
    is_chain = c == 1

    table_copy = pltpu.make_async_copy(table_ref, tab, tab_sem)
    table_copy.start()

    barrier = pltpu.get_barrier_semaphore()
    emb_section = 2 * c + seq // 16
    self_emb = is_chain & (zh == x) & (emb_section == x)

    def greet(to_seq, section, to):
        pl.semaphore_signal(
            barrier, inc=1, device_id=(to_seq, section, to), device_id_type=MESH
        )

    with jax.named_scope("greet"):
        @pl.loop(1, SEQ)
        def _(d):
            greet((seq + d) % SEQ, x, tp)

        @pl.loop(1, 16)
        def _(d):
            other = (4 * x + tp + d) % 16
            greet(seq, other // 4, other % 4)

        @pl.loop(0, NY)
        def _(b):
            @pl.when(jnp.logical_not(self_emb & (b == y)))
            def _():
                greet(NZ * b + x, emb_section, chain)

        @pl.when(is_chain)
        def _():
            @pl.loop(0, 16)
            def _(k):
                @pl.when(jnp.logical_not(self_emb & (k == seq % 16)))
                def _():
                    greet(16 * (x % 2) + k, zh, 2 * zl + x // 2)

    gain = gain_ref[:, pl.ds(pl.multiple_of(seq * ROWS, ROWS), ROWS)].astype(jnp.float32)
    gain = jnp.broadcast_to(gain, (ROWS, ROWS)).T

    def scaled(start):
        heads = qkv_ref[:, start : start + HEAD].astype(jnp.float32)
        return (heads * gain).astype(jnp.bfloat16)

    for j in range(2):
        for k, start in enumerate((2 * j, 2 * j + 1, 4 + j, 6 + j)):
            wsrc_ref[j, :, k * HEAD : (k + 1) * HEAD] = scaled(start * HEAD)
        wsrc_ref[j, :, SLICE:] = proj_ref[:, 2 * HEAD * j : 2 * HEAD * (j + 1)]
    ids_ref[:, :BLOCK] = jnp.broadcast_to(token_ref[...], (8, BLOCK))
    ids_ref[:, BLOCK:] = jnp.zeros((8, HEAD - BLOCK), jnp.int32)

    def x_copy(j):
        return remote(
            wsrc_ref.at[j], w.at[x, seq], x_send.at[j], x_recv.at[x], seq, 2 * c + j, comm
        )

    with jax.named_scope("barrier"):
        @pl.when(is_comm)
        def _():
            pl.semaphore_wait(barrier, 54)

        @pl.when(is_chain & jnp.logical_not(self_emb))
        def _():
            pl.semaphore_wait(barrier, 70)

        @pl.when(self_emb)
        def _():
            pl.semaphore_wait(barrier, 68)

    for j in range(2):
        stays = is_comm & (x == j)

        @pl.when(jnp.logical_not(stays))
        def _():
            x_copy(j).start()

        @pl.when(stays)
        def _():
            w[x, seq] = wsrc_ref[j]

    def ids_copy(d):
        return remote(
            ids_ref, ids_v.at[y], ids_send.at[d], ids_recv.at[y], (seq + d) % SEQ, x, tp
        )

    @pl.when(zh == x)
    def _():
        @pl.loop(1, SEQ)
        def _(d):
            ids_copy(d).start()

        ids_v[y] = ids_ref[...]

    def z_copy(layer, dz):
        return remote(
            w.at[layer, seq], w.at[layer, seq], z_send.at[layer], z_recv.at[layer, dz],
            NZ * y + (zh + dz) % NZ, x, comm,
        )

    def push(layer, s):
        remote(
            w.at[layer, s], w.at[layer, s], push_send.at[layer], push_recv.at[layer], seq, x, chain
        ).start()

    def y_copy(layer, way, step, zi, s):
        to = (seq + (NZ if way == 0 else SEQ - NZ)) % SEQ
        if step == 3:
            return remote(
                w.at[layer, s], w.at[layer, s], y_send.at[layer, way], push_recv.at[layer],
                to, x, chain,
            )
        return remote(
            w.at[layer, s], w.at[layer, s], y_send.at[layer, way], y_recv.at[layer, way, step, zi],
            to, x, comm,
        )

    def own_sends(layer):
        for zi in range(NZ):
            dz = Z_STEPS[zi]
            s = NZ * y + (zh + NZ - dz) % NZ
            if zi > 0:
                remote(
                    w.at[layer, s], w.at[layer, s], z_send.at[layer], z_recv.at[layer, dz],
                    seq, x, comm,
                ).wait_recv()
            for way in range(2):
                y_copy(layer, way, 0, zi, s).start()
            push(layer, s)

    def x_arrived(layer):
        local = (x == layer) & (x < 2)

        with jax.named_scope("x_wait"):
            @pl.when(jnp.logical_not(local))
            def _():
                remote(
                    w.at[layer, seq], w.at[layer, seq], x_send.at[0], x_recv.at[layer], seq, x, comm
                ).wait_recv()

    @pl.when(is_comm)
    def _():
        x_arrived(0)
        for dz in (1, 3, 2):
            z_copy(0, dz).start()
        with jax.named_scope("own_first"):
            own_sends(0)
        for layer in range(1, LAYERS):
            x_arrived(layer)

    with jax.named_scope("ids_wait"):
        @pl.loop(0, NY)
        def _(b):
            @pl.when(jnp.logical_not((zh == x) & (b == y)))
            def _():
                remote(
                    ids_ref, ids_v.at[b], ids_send.at[0], ids_recv.at[b], seq, x, tp
                ).wait_recv()

    with jax.named_scope("table_wait"):
        to_scalar = pltpu.make_async_copy(ids_v, ids_s, ids_local)
        to_scalar.start()
        to_scalar.wait()
        table_copy.wait()
    lane = lax.broadcasted_iota(jnp.int32, (32, HEAD), 1)
    ones = jnp.ones((HEAD, HEAD), jnp.bfloat16)

    def emb_copy(b):
        return remote(
            emb_out.at[b], emb_in.at[seq % 16], emb_send.at[b], emb_recv.at[seq % 16],
            NZ * b + x, emb_section, chain,
        )

    def emb_self(b):
        return self_emb & (b == y)

    with jax.named_scope("gather"):
        @pl.loop(0, NY)
        def _(b):
            def tokens(i, got):
                picked = []
                for k in range(8):
                    v = ids_s[b, 0, 8 * i + k]
                    tile = tab[:, v >> 7].reshape(32, HEAD)
                    picked.append(jnp.where(lane == (v & 127), tile, jnp.zeros_like(tile)))
                spread = jnp.dot(
                    jnp.concatenate(picked, axis=0), ones, preferred_element_type=jnp.float32
                )
                for k in range(8):
                    got = jnp.where(lane == 8 * i + k, spread[32 * k : 32 * (k + 1)], got)
                return got

            got = lax.fori_loop(0, 8, tokens, jnp.zeros((32, HEAD), jnp.float32))
            emb_out[b] = got.astype(jnp.bfloat16)

            @pl.when(jnp.logical_not(emb_self(b)))
            def _():
                emb_copy(b).start()

            @pl.when(emb_self(b))
            def _():
                emb_in[seq % 16] = got.astype(jnp.bfloat16)

    def received(way, step, zi):
        row = (y + (NY - step if way == 0 else step)) % NY
        return NZ * row + (zh + NZ - Z_STEPS[zi]) % NZ

    def arrived(layer, way, step, zi):
        s = received(way, step, zi)
        y_copy(layer, way, step - 1, zi, s).wait_recv()
        return s

    @pl.when(is_comm)
    def _():
        @pl.loop(0, LAYERS)
        def _(layer):
            @pl.when(layer < LAYERS - 1)
            def _():
                for dz in (1, 3, 2):
                    z_copy(layer + 1, dz).start()

            with jax.named_scope("ring"):
                for step in range(1, 4):
                    for zi in range(NZ):
                        for way in range(2):
                            s = arrived(layer, way, step, zi)
                            if step < 3 or (zi < 2) == (way == 0):
                                y_copy(layer, way, step, zi, s).start()
                            push(layer, s)

            with jax.named_scope("own_next"):
                @pl.when(layer < LAYERS - 1)
                def _():
                    own_sends(layer + 1)

        @pl.loop(0, LAYERS)
        def _(layer):
            for way in range(2):
                remote(
                    w.at[layer, pl.ds(0, 14)], w.at[layer, pl.ds(0, 14)], y_send.at[layer, way],
                    y_recv.at[layer, way, 0, 0], seq, x, comm,
                ).wait_send()
            remote(
                w.at[layer, pl.ds(0, 3)], w.at[layer, pl.ds(0, 3)], z_send.at[layer],
                z_recv.at[layer, 1], seq, x, comm,
            ).wait_send()
            remote(
                w.at[layer, pl.ds(0, 28)], w.at[layer, pl.ds(0, 28)], push_send.at[layer],
                push_recv.at[layer], seq, x, chain,
            ).wait_send()

    def member(d):
        other = m ^ d
        return other, other % 4, 2 * (other // 4) + 1

    def ag_copy(layer, d):
        _, section, to = member(d)
        return remote(
            hid.at[layer, m], hid.at[layer, m], ag_send.at[layer], ag_recv.at[layer, m],
            seq, section, to,
        )

    def rs_copy(layer, d):
        other, section, to = member(d)
        return remote(
            part_out.at[layer, other], part_in.at[layer, m], rs_send.at[layer],
            rs_recv.at[layer, m], seq, section, to,
        )

    def kv_copy(layer, src, i, to):
        return remote(src, akv.at[layer], kv_send.at[layer, i], kv_recv.at[layer], to, x, tp)

    def out_copy(layer):
        return remote(
            hid.at[layer + 1, m], out_ref.at[:, pl.ds(pl.multiple_of((x % 2) * SLICE, SLICE), SLICE)],
            out_send.at[layer], out_recv.at[x % 2], seq, layer, 2 * zl + x // 2,
        )

    def out_self(layer):
        return (layer == x) & (x >= 2)

    @pl.when(is_chain)
    def _():
        with jax.named_scope("emb_wait"):
            @pl.loop(0, 16)
            def _(k):
                @pl.when(jnp.logical_not(self_emb & (k == seq % 16)))
                def _():
                    remote(
                        emb_out.at[0], emb_in.at[k], emb_send.at[0], emb_recv.at[k], seq, x, tp
                    ).wait_recv()

        start = emb_in[...].reshape(SLICE, HEAD).astype(jnp.float32).T[:BLOCK]
        res[...] = start
        hid[0, m] = start.astype(jnp.bfloat16)
        for d in range(1, GROUP):
            ag_copy(0, d).start()

        a = rope_a_ref[pl.ds(seq, 1), :]
        cos_a, sin_a = a[:, :HEAD], a[:, HEAD:]
        cos_b, sin_b = rope_b_ref[:, :HEAD], rope_b_ref[:, HEAD:]
        cosine = cos_a * cos_b - sin_a * sin_b
        sine = sin_a * cos_b + cos_a * sin_b
        side = lax.broadcasted_iota(jnp.int32, (BLOCK, HEAD), 1)
        sine = jnp.where(side < HEAD // 2, -sine, sine)

        def rotated(v):
            return (v * cosine + pltpu.roll(v, HEAD // 2, 1) * sine).astype(jnp.bfloat16)

        row = lax.broadcasted_iota(jnp.int32, (2 * BLOCK, 2 * BLOCK), 0) % BLOCK
        col = lax.broadcasted_iota(jnp.int32, (2 * BLOCK, 2 * BLOCK), 1)
        allowed = ((col < BLOCK) & (seq > 0)) | ((col >= BLOCK) & (col - BLOCK <= row))

        @pl.loop(0, LAYERS)
        def _(layer):
            with jax.named_scope("w_wait"):
                remote(
                    w.at[layer], w.at[layer], push_send.at[layer], push_recv.at[layer], seq, x, chain
                ).wait_recv()

            def add(d, square):
                other = m ^ d

                @pl.when(d > 0)
                def _():
                    remote(
                        hid.at[layer, other], hid.at[layer, other], ag_send.at[layer],
                        ag_recv.at[layer, other], seq, x, chain,
                    ).wait_recv()

                h = hid[layer, other]
                weights = w[layer, pl.ds(4 * other, 4), :, :SLICE].reshape(SLICE, SLICE)
                product = jnp.dot(h, weights, preferred_element_type=jnp.float32)

                @pl.when(d == 0)
                def _():
                    acc[...] = product

                @pl.when(d > 0)
                def _():
                    acc[...] += product

                hf = h.astype(jnp.float32)
                return square + jnp.sum(hf * hf, axis=1, keepdims=True)

            with jax.named_scope("ag_qkv"):
                square = lax.fori_loop(0, GROUP, add, jnp.zeros((BLOCK, 1), jnp.float32))
            projected = acc[...] * lax.rsqrt(square * (1.0 / (GROUP * SLICE)) + EPS)
            q0 = rotated(projected[:, :HEAD])
            q1 = rotated(projected[:, HEAD : 2 * HEAD])
            key = rotated(projected[:, 2 * HEAD : 3 * HEAD])
            value = projected[:, 3 * HEAD :].astype(jnp.bfloat16)
            kv[layer, :, :HEAD] = key
            kv[layer, :, HEAD:] = value

            @pl.when(seq == 0)
            def _():
                for i in range(1, NY):
                    kv_copy(layer, kv.at[layer], i, NZ * i).start()
                for i in range(1, NZ):
                    kv_copy(layer, kv.at[layer], NY + i, i).start()
                akv[layer, :, :HEAD] = key
                akv[layer, :, HEAD:] = value

            with jax.named_scope("kv_wait"):
                @pl.when(seq > 0)
                def _():
                    kv_copy(layer, kv.at[layer], 0, seq).wait_recv()

                    @pl.when(zh == 0)
                    def _():
                        for i in range(1, NZ):
                            kv_copy(layer, akv.at[layer], NY + i, seq + i).start()

            queries = jnp.concatenate([q0, q1], axis=0)
            keys = jnp.concatenate([akv[layer, :, :HEAD], key], axis=0)
            values = jnp.concatenate([akv[layer, :, HEAD:], value], axis=0)
            scores = lax.dot_general(
                queries, keys, (((1,), (1,)), ((), ())), preferred_element_type=jnp.float32
            ) * (HEAD ** -0.5)
            scores = jnp.where(allowed, scores, MASKED)
            e = jnp.exp(scores - jnp.max(scores, axis=1, keepdims=True))
            probs = (e / jnp.sum(e, axis=1, keepdims=True)).astype(jnp.bfloat16)
            both = jnp.dot(probs, values, preferred_element_type=jnp.float32).astype(jnp.bfloat16)
            attended = jnp.concatenate([both[:BLOCK], both[BLOCK:]], axis=1)

            def partial(other):
                weights = w[layer, pl.ds(4 * other, 4), :, SLICE:].reshape(SLICE, 2 * HEAD)
                return lax.dot_general(
                    attended, weights, (((1,), (1,)), ((), ())), preferred_element_type=jnp.float32
                )

            with jax.named_scope("partials"):
                @pl.loop(1, GROUP)
                def _(d):
                    other = m ^ d
                    part_out[layer, other] = partial(other).astype(jnp.bfloat16)
                    rs_copy(layer, d).start()

                acc[...] = partial(m)

            with jax.named_scope("rs_wait"):
                @pl.loop(1, GROUP)
                def _(d):
                    other = m ^ d
                    remote(
                        part_out.at[layer, other], part_in.at[layer, other], rs_send.at[layer],
                        rs_recv.at[layer, other], seq, x, chain,
                    ).wait_recv()
                    acc[...] += part_in[layer, other].astype(jnp.float32)

            new = (res[...] + acc[...]).astype(jnp.bfloat16)
            res[...] = new.astype(jnp.float32)
            hid[layer + 1, m] = new

            @pl.when(layer < LAYERS - 1)
            def _():
                for d in range(1, GROUP):
                    ag_copy(layer + 1, d).start()

            @pl.when(jnp.logical_not(out_self(layer)))
            def _():
                out_copy(layer).start()

            @pl.when(out_self(layer))
            def _():
                out_ref[:, pl.ds(pl.multiple_of((x % 2) * SLICE, SLICE), SLICE)] = new

        @pl.loop(0, LAYERS)
        def _(layer):
            remote(
                hid.at[layer, pl.ds(0, 7)], hid.at[layer, pl.ds(0, 7)], ag_send.at[layer],
                ag_recv.at[layer, 0], seq, x, chain,
            ).wait_send()
            remote(
                part_out.at[layer, pl.ds(0, 7)], part_in.at[layer, pl.ds(0, 7)], rs_send.at[layer],
                rs_recv.at[layer, 0], seq, x, chain,
            ).wait_send()

            @pl.when(seq == 0)
            def _():
                for i in range(1, NY):
                    kv_copy(layer, kv.at[layer], i, seq).wait_send()

            @pl.when(zh == 0)
            def _():
                for i in range(1, NZ):
                    kv_copy(layer, kv.at[layer], NY + i, seq).wait_send()

            @pl.when(jnp.logical_not(out_self(layer)))
            def _():
                out_copy(layer).wait_send()

    for j in range(2):
        @pl.when(jnp.logical_not(is_comm & (x == j)))
        def _():
            x_copy(j).wait_send()

    @pl.when(zh == x)
    def _():
        @pl.loop(1, SEQ)
        def _(d):
            ids_copy(d).wait_send()

    @pl.loop(0, NY)
    def _(b):
        @pl.when(jnp.logical_not(emb_self(b)))
        def _():
            emb_copy(b).wait_send()

    for half in range(2):
        @pl.when(jnp.logical_not(is_chain & (x == 2 + half)))
        def _():
            remote(
                hid.at[0, 0], out_ref.at[:, pl.ds(half * SLICE, SLICE)], out_send.at[0],
                out_recv.at[half], seq, x, tp,
            ).wait_recv()


def rope_constants():
    half = np.arange(HEAD // 2, dtype=np.float64)
    freq = np.float64(ROPE_BASE) ** (-2.0 * half / HEAD)
    freq = np.concatenate([freq, freq])
    coarse = np.arange(SEQ, dtype=np.float64)[:, None] * BLOCK * freq[None]
    fine = np.arange(BLOCK, dtype=np.float64)[:, None] * freq[None]
    pair = lambda angle: np.concatenate([np.cos(angle), np.sin(angle)], axis=1).astype(np.float32)
    return pair(coarse), pair(fine)


def body(token_ids, embed_columns, norm_gain, qkv_weight, out_weight):
    features, vocabulary = embed_columns.shape
    table = embed_columns.reshape(features // 8, 8, vocabulary // HEAD, HEAD).transpose(0, 2, 1, 3)
    rope_a, rope_b = rope_constants()
    bf16, f32 = jnp.bfloat16, jnp.float32
    vmem = pl.BlockSpec(memory_space=pltpu.VMEM)
    dma = pltpu.SemaphoreType.DMA
    states = pl.pallas_call(
        kernel,
        out_shape=jax.ShapeDtypeStruct((BLOCK, 2 * SLICE), bf16),
        in_specs=[vmem, pl.BlockSpec(memory_space=pl.ANY), vmem, vmem, vmem, vmem, vmem],
        out_specs=vmem,
        scratch_shapes=[
            pltpu.VMEM((8, HEAD), jnp.int32),
            pltpu.VMEM((2, ROWS, WIDE), bf16),
            pltpu.VMEM((LAYERS, SEQ, ROWS, WIDE), bf16),
            pltpu.VMEM(table.shape, bf16),
            pltpu.VMEM((NY, 8, HEAD), jnp.int32),
            pltpu.SMEM((NY, 8, HEAD), jnp.int32),
            pltpu.VMEM((NY, 32, HEAD), bf16),
            pltpu.VMEM((16, 32, HEAD), bf16),
            pltpu.VMEM((LAYERS + 1, GROUP, BLOCK, SLICE), bf16),
            pltpu.VMEM((LAYERS, GROUP, BLOCK, SLICE), bf16),
            pltpu.VMEM((LAYERS, GROUP, BLOCK, SLICE), bf16),
            pltpu.VMEM((LAYERS, BLOCK, 2 * HEAD), bf16),
            pltpu.VMEM((LAYERS, BLOCK, 2 * HEAD), bf16),
            pltpu.VMEM((BLOCK, SLICE), f32),
            pltpu.VMEM((BLOCK, SLICE), f32),
            dma((2,)),
            dma((LAYERS,)),
            dma((LAYERS,)),
            dma((LAYERS, NZ)),
            dma((LAYERS, 2)),
            dma((LAYERS, 2, 3, NZ)),
            dma((LAYERS,)),
            dma((LAYERS,)),
            dma((SEQ,)),
            dma((NY,)),
            dma,
            dma,
            dma((NY,)),
            dma((16,)),
            dma((LAYERS,)),
            dma((LAYERS, GROUP)),
            dma((LAYERS,)),
            dma((LAYERS, GROUP)),
            dma((LAYERS, NY + NZ)),
            dma((LAYERS,)),
            dma((LAYERS,)),
            dma((2,)),
        ],
        compiler_params=pltpu.CompilerParams(
            collective_id=0, has_side_effects=True, vmem_limit_bytes=62 * 1024 * 1024
        ),
    )(
        token_ids[None], table, norm_gain, qkv_weight[0], out_weight[0],
        jnp.asarray(rope_a), jnp.asarray(rope_b),
    )
    return states[None]


def solution(mesh):
    placed = (
        P("seq"),
        P(("tp", "seq"), None),
        P("section", None),
        P("section", "seq", "tp"),
        P("section", "seq", "tp"),
    )
    return jax.shard_map(
        body, mesh=mesh, in_specs=placed, out_specs=P("section", "seq", "tp"), check_vma=False
    )
```

```python
import functools

import jax
import jax.numpy as jnp
import numpy as np
from jax import lax
from jax.experimental import pallas as pl
from jax.experimental.pallas import tpu as pltpu
from jax.sharding import PartitionSpec as P

MESH = pl.DeviceIdType.MESH
LAYERS = 4
NY = 8
NZ = 4
SEQ = NY * NZ
GROUP = 8
ROWS = 128
BLOCK = 64
HEAD = 128
FIRST = 112
SLICE = 512
EPS = 1e-05
ROPE_BASE = 500000.0
MASKED = -1e30
Z_STEPS = (0, 3, 1, 2)


def remote(src, dst, send, recv, seq, section, tp):
    return pltpu.make_async_remote_copy(
        src_ref=src,
        dst_ref=dst,
        send_sem=send,
        recv_sem=recv,
        device_id=(seq, section, tp),
        device_id_type=MESH,
    )


def kernel(
    token_ref, table_ref, gain_ref, qkv_ref, proj_ref, rope_a_ref, rope_b_ref, out_ref,
    ids_ref, src_q, src_o, wq, wo, tab, tab_lent, ids_v, ids_s, emb_out, emb_in, hid, part_out, part_in,
    kv, akv, acc, res,
    x_send, x_recv, za_send, za_recv, zb_send, ya_send, ya_recv, yb_send, yb_recv,
    push_send, push_recv, ids_send, ids_recv, ids_local, tab_sem, lent_send, lent_recv,
    emb_send, emb_recv, ag_send, ag_recv, rs_send, rs_recv, kv_send, kv_recv, out_send, out_recv,
):
    seq = lax.axis_index("seq")
    x = lax.axis_index("section")
    tp = lax.axis_index("tp")
    y = seq // NZ
    zh = seq % NZ
    zl = tp // 2
    c = tp % 2
    m = 4 * zl + x
    comm = 2 * zl
    chain = 2 * zl + 1
    is_comm = c == 0
    is_chain = c == 1

    parts = (wq, wo)
    sources = (src_q, src_o)
    table_copy = pltpu.make_async_copy(table_ref, tab, tab_sem)
    lent_table = remote(table_ref, tab_lent, lent_send, lent_recv, seq, x, chain)

    @pl.when(is_chain)
    def _():
        table_copy.start()

    barrier = pltpu.get_barrier_semaphore()
    self_emb = (zh == x) & (seq // 16 == x % 2)

    def greet(to_seq, section, to):
        pl.semaphore_signal(
            barrier, inc=1, device_id=(to_seq, section, to), device_id_type=MESH
        )

    with jax.named_scope("greet"):
        @pl.loop(1, SEQ)
        def _(d):
            greet((seq + d) % SEQ, x, tp)

        @pl.loop(1, 16)
        def _(d):
            other = (4 * x + tp + d) % 16
            greet(seq, other // 4, other % 4)

        @pl.loop(1, NZ)
        def _(dz):
            greet(NZ * y + (zh + dz) % NZ, x, 2 * zl + 1 - c)

        @pl.when(is_chain)
        def _():
            @pl.loop(0, 16)
            def _(k):
                @pl.when(jnp.logical_not(self_emb & (k == 8 * (x // 2) + y)))
                def _():
                    greet(NZ * (k % NY) + x, 2 * (k // NY) + seq // 16, chain)

                @pl.when(jnp.logical_not(self_emb & (k == seq % 16)))
                def _():
                    greet(16 * (x % 2) + k, zh, chain)

    gain = gain_ref[:, pl.ds(pl.multiple_of(seq * ROWS, ROWS), ROWS)].astype(jnp.float32)
    gain = jnp.broadcast_to(gain, (ROWS, ROWS)).T

    def scaled(start):
        heads = qkv_ref[:, start : start + HEAD].astype(jnp.float32)
        return (heads * gain).astype(jnp.bfloat16)

    for j in range(2):
        for k, start in enumerate((2 * j, 2 * j + 1, 4 + j, 6 + j)):
            src_q[j, :, k * HEAD : (k + 1) * HEAD] = scaled(start * HEAD)
        src_o[j] = proj_ref[:, 2 * HEAD * j : 2 * HEAD * (j + 1)]
    ids_ref[:, :BLOCK] = jnp.broadcast_to(token_ref[...], (8, BLOCK))
    ids_ref[:, BLOCK:] = jnp.zeros((8, HEAD - BLOCK), jnp.int32)

    def x_copy(part, j):
        return remote(
            sources[part].at[j], parts[part].at[x, seq], x_send.at[part, j], x_recv.at[x, part],
            seq, 2 * c + j, comm,
        )

    with jax.named_scope("barrier"):
        @pl.when(is_comm)
        def _():
            pl.semaphore_wait(barrier, 49)

        @pl.when(is_chain & jnp.logical_not(self_emb))
        def _():
            pl.semaphore_wait(barrier, 81)

        @pl.when(is_chain & self_emb)
        def _():
            pl.semaphore_wait(barrier, 79)

    for part in range(2):
        for j in range(2):
            stays = is_comm & (x == j)

            @pl.when(jnp.logical_not(stays))
            def _():
                x_copy(part, j).start()

            @pl.when(stays)
            def _():
                parts[part][x, seq] = sources[part][j]

    def ids_copy(d):
        return remote(
            ids_ref, ids_v.at[y], ids_send.at[d], ids_recv.at[y], (seq + d) % SEQ, x, tp
        )

    @pl.when(is_chain & (zh == x))
    def _():
        @pl.loop(1, SEQ)
        def _(d):
            ids_copy(d).start()

        ids_v[y] = ids_ref[...]

    def early(part, layer, s):
        return parts[part].at[layer, s, pl.ds(0, FIRST)]

    def late(part, layer, s):
        return parts[part].at[layer, s, pl.ds(FIRST, ROWS - FIRST)]

    def beside(way):
        return (seq + (NZ if way == 0 else SEQ - NZ)) % SEQ

    def za_copy(part, layer, dz, s):
        ref = early(part, layer, s)
        return remote(
            ref, ref, za_send.at[layer, part], za_recv.at[layer, part, dz],
            NZ * y + (zh + dz) % NZ, x, comm,
        )

    def ya_copy(part, layer, way, step, zi, s):
        ref = early(part, layer, s)
        if step == 3:
            return remote(
                ref, ref, ya_send.at[layer, part, way], push_recv.at[layer, part],
                beside(way), x, chain,
            )
        return remote(
            ref, ref, ya_send.at[layer, part, way], ya_recv.at[layer, part, way, step, zi],
            beside(way), x, comm,
        )

    def yb_copy(part, layer, way, step, s):
        ref = late(part, layer, s)
        return remote(
            ref, ref, yb_send.at[layer, part, way],
            yb_recv.at[layer, part, 6 if step == 3 else 3 * way + step], beside(way), x, comm,
        )

    def zb_sends(part, layer, s):
        ref = late(part, layer, s)
        for dz in (1, 3, 2):
            remote(
                ref, ref, zb_send.at[layer, part], push_recv.at[layer, part],
                NZ * y + (zh + dz) % NZ, x, chain,
            ).start()

    def push(kind, part, layer, ref):
        remote(
            ref, ref, push_send.at[layer, part, kind], push_recv.at[layer, part], seq, x, chain
        ).start()

    def x_arrived(part, layer, first=False):
        local = (x == layer) & (x < 2)
        ref = parts[part].at[layer, seq]

        with jax.named_scope("x_wait"):
            @pl.when(jnp.logical_not(local))
            def _():
                remote(
                    ref, ref, x_send.at[0, 0], x_recv.at[layer, part], seq, x, comm
                ).wait_recv()

        for dz in (1, 3, 2) if first else (3, 1):
            za_copy(part, layer, dz, seq).start()

    def z_forward(part, layer):
        s = NZ * y + (zh + 1) % NZ
        za_copy(part, layer, 3, s).wait_recv()
        ref = early(part, layer, s)
        remote(
            ref, ref, za_send.at[layer, part], za_recv.at[layer, part, 2],
            NZ * y + (zh + 3) % NZ, x, comm,
        ).start()

    def own_start(part, layer):
        for way in range(2):
            yb_copy(part, layer, way, 0, seq).start()
        for way in range(2):
            ya_copy(part, layer, way, 0, 0, seq).start()
        zb_sends(part, layer, seq)
        push(0, part, layer, parts[part].at[layer, seq])

    def own_rest(part, layer, first=False):
        for zi in range(1, NZ):
            dz = Z_STEPS[zi]
            s = NZ * y + (zh + NZ - dz) % NZ
            if dz != 3 or first:
                za_copy(part, layer, dz, s).wait_recv()
            for way in range(2):
                ya_copy(part, layer, way, 0, zi, s).start()
            push(1, part, layer, early(part, layer, s))

    def row_from(way, step):
        return (y + (NY - step if way == 0 else step)) % NY

    def ring_late(part, layer, step):
        for way in range(2):
            s = NZ * row_from(way, step) + zh
            yb_copy(part, layer, way, step - 1, s).wait_recv()
            if step < 3:
                yb_copy(part, layer, way, step, s).start()
            else:
                @pl.when(zh % 2 == way)
                def _():
                    yb_copy(part, layer, way, 3, s).start()
            zb_sends(part, layer, s)
            push(2, part, layer, late(part, layer, s))

    def ring(part, layer, step):
        for zi in range(NZ):
            for way in range(2):
                s = NZ * row_from(way, step) + (zh + NZ - Z_STEPS[zi]) % NZ
                ya_copy(part, layer, way, step - 1, zi, s).wait_recv()
                if step < 3 or (zi < 2) == (way == 0):
                    ya_copy(part, layer, way, step, zi, s).start()
                push(1, part, layer, early(part, layer, s))

    def across(part, layer):
        s = NZ * ((y + NY // 2) % NY) + zh
        yb_copy(part, layer, 0, 3, s).wait_recv()
        zb_sends(part, layer, s)
        push(2, part, layer, late(part, layer, s))

    def relay(part, layer):
        last = layer == LAYERS - 1

        def unless_last(step):
            if part == 0:
                step(1, layer)
            else:
                @pl.when(jnp.logical_not(last))
                def _():
                    step(0, layer + 1)

        def own(part, layer):
            own_start(part, layer)
            own_rest(part, layer)

        with jax.named_scope("late1"):
            ring_late(part, layer, 1)
        with jax.named_scope("step1"):
            ring(part, layer, 1)
        with jax.named_scope("zfwd"):
            unless_last(z_forward)
        with jax.named_scope("late2"):
            ring_late(part, layer, 2)
        with jax.named_scope("step2"):
            ring(part, layer, 2)
        with jax.named_scope("late3"):
            ring_late(part, layer, 3)
        with jax.named_scope("own"):
            unless_last(own)

        @pl.when(layer < LAYERS - 1 - part)
        def _():
            x_arrived(1 - part, layer + 1 + part)

        with jax.named_scope("step3"):
            ring(part, layer, 3)
        with jax.named_scope("across"):
            across(part, layer)

    @pl.when(is_comm)
    def _():
        x_arrived(0, 0, True)
        with jax.named_scope("own_first"):
            own_start(0, 0)
            lent_table.start()
            x_arrived(1, 0)
            own_rest(0, 0, True)
            x_arrived(0, 1)

        @pl.loop(0, LAYERS)
        def _(layer):
            relay(0, layer)
            relay(1, layer)

        @pl.loop(0, LAYERS)
        def _(layer):
            for part in range(2):
                def sent(sem, block):
                    remote(block, block, sem, push_recv.at[layer, part], seq, x, chain).wait_send()

                def early_sent(sem, count):
                    sent(sem, parts[part].at[layer, pl.ds(0, count), pl.ds(0, FIRST)])

                def late_sent(sem, count):
                    sent(sem, parts[part].at[layer, pl.ds(0, count), pl.ds(FIRST, ROWS - FIRST)])

                early_sent(za_send.at[layer, part], 3)
                late_sent(zb_send.at[layer, part], 24)
                sent(push_send.at[layer, part, 0], parts[part].at[layer, 0])
                early_sent(push_send.at[layer, part, 1], 27)
                late_sent(push_send.at[layer, part, 2], 7)
                for way in range(2):
                    early_sent(ya_send.at[layer, part, way], 14)

                    @pl.when(zh % 2 == way)
                    def _():
                        late_sent(yb_send.at[layer, part, way], 4)

                    @pl.when(zh % 2 != way)
                    def _():
                        late_sent(yb_send.at[layer, part, way], 3)

        lent_table.wait_send()

    lane = lax.broadcasted_iota(jnp.int32, (32, HEAD), 1)

    def emb_copy(k):
        return remote(
            emb_out.at[k], emb_in.at[seq % 16], emb_send.at[k], emb_recv.at[seq % 16],
            NZ * (k % NY) + x, 2 * (k // NY) + seq // 16, chain,
        )

    def emb_self(k):
        return self_emb & (k == NY * (x // 2) + y)

    @pl.when(is_chain)
    def _():
        with jax.named_scope("ids_wait"):
            @pl.loop(0, NY)
            def _(b):
                @pl.when(jnp.logical_not((zh == x) & (b == y)))
                def _():
                    remote(
                        ids_ref, ids_v.at[b], ids_send.at[0], ids_recv.at[b], seq, x, tp
                    ).wait_recv()

        with jax.named_scope("table_wait"):
            to_scalar = pltpu.make_async_copy(ids_v, ids_s, ids_local)
            to_scalar.start()
            to_scalar.wait()
            table_copy.wait()

        with jax.named_scope("gather"):
            def look_up(columns, k, b):
                def token(i, got):
                    v = ids_s[b, 0, i]
                    tile = columns[:, v >> 7].reshape(32, HEAD).astype(jnp.float32)
                    column = jnp.sum(
                        jnp.where(lane == (v & 127), tile, 0.0), axis=1, keepdims=True
                    )
                    return jnp.where(lane == i, column, got)

                got = lax.fori_loop(0, BLOCK, token, jnp.zeros((32, HEAD), jnp.float32), unroll=8)
                emb_out[k] = got.astype(jnp.bfloat16)

                @pl.when(jnp.logical_not(emb_self(k)))
                def _():
                    emb_copy(k).start()

                @pl.when(emb_self(k))
                def _():
                    emb_in[seq % 16] = got.astype(jnp.bfloat16)

            @pl.loop(0, NY)
            def _(b):
                look_up(tab, NY + b, b)

            lent_table.wait_recv()

            @pl.loop(0, NY)
            def _(b):
                look_up(tab_lent, b, b)

    def member(d):
        other = m ^ d
        return other, other % 4, 2 * (other // 4) + 1

    def ag_copy(layer, d):
        _, section, to = member(d)
        return remote(
            hid.at[layer, m], hid.at[layer, m], ag_send.at[layer], ag_recv.at[layer, m],
            seq, section, to,
        )

    def rs_copy(layer, d):
        other, section, to = member(d)
        return remote(
            part_out.at[layer, other], part_in.at[layer, m], rs_send.at[layer],
            rs_recv.at[layer, m], seq, section, to,
        )

    def kv_copy(layer, src, i, to):
        return remote(src, akv.at[layer], kv_send.at[layer, i], kv_recv.at[layer], to, x, tp)

    def out_copy(layer):
        return remote(
            hid.at[layer + 1, m], out_ref.at[:, pl.ds(pl.multiple_of((x % 2) * SLICE, SLICE), SLICE)],
            out_send.at[layer], out_recv.at[x % 2], seq, layer, 2 * zl + x // 2,
        )

    def out_self(layer):
        return (layer == x) & (x >= 2)

    @pl.when(is_chain)
    def _():
        with jax.named_scope("emb_wait"):
            @pl.loop(0, 16)
            def _(k):
                @pl.when(jnp.logical_not(self_emb & (k == seq % 16)))
                def _():
                    remote(
                        emb_out.at[0], emb_in.at[k], emb_send.at[0], emb_recv.at[k], seq, x, tp
                    ).wait_recv()

        start = emb_in[...].reshape(SLICE, HEAD).astype(jnp.float32).T[:BLOCK]
        res[...] = start
        hid[0, m] = start.astype(jnp.bfloat16)
        for d in range(1, GROUP):
            ag_copy(0, d).start()

        a = rope_a_ref[pl.ds(seq, 1), :]
        cos_a, sin_a = a[:, :HEAD], a[:, HEAD:]
        cos_b, sin_b = rope_b_ref[:, :HEAD], rope_b_ref[:, HEAD:]
        cosine = cos_a * cos_b - sin_a * sin_b
        sine = sin_a * cos_b + cos_a * sin_b
        side = lax.broadcasted_iota(jnp.int32, (BLOCK, HEAD), 1)
        sine = jnp.where(side < HEAD // 2, -sine, sine)

        def rotated(v):
            return (v * cosine + pltpu.roll(v, HEAD // 2, 1) * sine).astype(jnp.bfloat16)

        row = lax.broadcasted_iota(jnp.int32, (2 * BLOCK, 2 * BLOCK), 0) % BLOCK
        col = lax.broadcasted_iota(jnp.int32, (2 * BLOCK, 2 * BLOCK), 1)
        allowed = ((col < BLOCK) & (seq > 0)) | ((col >= BLOCK) & (col - BLOCK <= row))

        @pl.loop(0, LAYERS)
        def _(layer):
            with jax.named_scope("w_wait"):
                remote(
                    wq.at[layer], wq.at[layer], x_send.at[0, 0], push_recv.at[layer, 0], seq, x, chain
                ).wait_recv()

            def add(d, square):
                other = m ^ d

                @pl.when(d > 0)
                def _():
                    remote(
                        hid.at[layer, other], hid.at[layer, other], ag_send.at[layer],
                        ag_recv.at[layer, other], seq, x, chain,
                    ).wait_recv()

                h = hid[layer, other]
                add_product(d, h, other, 2 * HEAD)
                hf = h.astype(jnp.float32)
                return square + jnp.sum(hf * hf, axis=1, keepdims=True)

            def add_product(d, h, other, at):
                weights = wq[layer, pl.ds(4 * other, 4), :, at : at + 2 * HEAD]
                product = jnp.dot(
                    h, weights.reshape(SLICE, 2 * HEAD), preferred_element_type=jnp.float32
                )

                @pl.when(d == 0)
                def _():
                    acc[:, at : at + 2 * HEAD] = product

                @pl.when(d > 0)
                def _():
                    acc[:, at : at + 2 * HEAD] += product

            with jax.named_scope("ag_qkv"):
                square = lax.fori_loop(0, GROUP, add, jnp.zeros((BLOCK, 1), jnp.float32))
            scale = lax.rsqrt(square * (1.0 / (GROUP * SLICE)) + EPS)
            key = rotated(acc[:, 2 * HEAD : 3 * HEAD] * scale)
            value = (acc[:, 3 * HEAD :] * scale).astype(jnp.bfloat16)
            kv[layer, :, :HEAD] = key
            kv[layer, :, HEAD:] = value

            @pl.when(seq == 0)
            def _():
                for i in range(1, NY):
                    kv_copy(layer, kv.at[layer], i, NZ * i).start()
                for i in range(1, NZ):
                    kv_copy(layer, kv.at[layer], NY + i, i).start()
                akv[layer, :, :HEAD] = key
                akv[layer, :, HEAD:] = value

            with jax.named_scope("queries"):
                @pl.loop(0, GROUP)
                def _(d):
                    other = m ^ d
                    add_product(d, hid[layer, other], other, 0)

            q0 = rotated(acc[:, :HEAD] * scale)
            q1 = rotated(acc[:, HEAD : 2 * HEAD] * scale)

            with jax.named_scope("kv_wait"):
                @pl.when(seq > 0)
                def _():
                    kv_copy(layer, kv.at[layer], 0, seq).wait_recv()

                    @pl.when(zh == 0)
                    def _():
                        for i in range(1, NZ):
                            kv_copy(layer, akv.at[layer], NY + i, seq + i).start()

            queries = jnp.concatenate([q0, q1], axis=0)
            keys = jnp.concatenate([akv[layer, :, :HEAD], key], axis=0)
            values = jnp.concatenate([akv[layer, :, HEAD:], value], axis=0)
            scores = lax.dot_general(
                queries, keys, (((1,), (1,)), ((), ())), preferred_element_type=jnp.float32
            ) * (HEAD ** -0.5)
            scores = jnp.where(allowed, scores, MASKED)
            e = jnp.exp(scores - jnp.max(scores, axis=1, keepdims=True))
            probs = (e / jnp.sum(e, axis=1, keepdims=True)).astype(jnp.bfloat16)
            both = jnp.dot(probs, values, preferred_element_type=jnp.float32).astype(jnp.bfloat16)
            attended = jnp.concatenate([both[:BLOCK], both[BLOCK:]], axis=1)

            def partial(other):
                weights = wo[layer, pl.ds(4 * other, 4)].reshape(SLICE, 2 * HEAD)
                return lax.dot_general(
                    attended, weights, (((1,), (1,)), ((), ())), preferred_element_type=jnp.float32
                )

            with jax.named_scope("o_wait"):
                remote(
                    wo.at[layer], wo.at[layer], x_send.at[0, 0], push_recv.at[layer, 1], seq, x, chain
                ).wait_recv()

            with jax.named_scope("partials"):
                @pl.loop(1, GROUP)
                def _(d):
                    other = m ^ d
                    part_out[layer, other] = partial(other).astype(jnp.bfloat16)
                    rs_copy(layer, d).start()

                acc[...] = partial(m)

            with jax.named_scope("rs_wait"):
                @pl.loop(1, GROUP)
                def _(d):
                    other = m ^ d
                    remote(
                        part_out.at[layer, other], part_in.at[layer, other], rs_send.at[layer],
                        rs_recv.at[layer, other], seq, x, chain,
                    ).wait_recv()
                    acc[...] += part_in[layer, other].astype(jnp.float32)

            new = (res[...] + acc[...]).astype(jnp.bfloat16)
            res[...] = new.astype(jnp.float32)
            hid[layer + 1, m] = new

            @pl.when(layer < LAYERS - 1)
            def _():
                for d in range(1, GROUP):
                    ag_copy(layer + 1, d).start()

            @pl.when(jnp.logical_not(out_self(layer)))
            def _():
                out_copy(layer).start()

            @pl.when(out_self(layer))
            def _():
                out_ref[:, pl.ds(pl.multiple_of((x % 2) * SLICE, SLICE), SLICE)] = new

        @pl.loop(0, LAYERS)
        def _(layer):
            remote(
                hid.at[layer, pl.ds(0, 7)], hid.at[layer, pl.ds(0, 7)], ag_send.at[layer],
                ag_recv.at[layer, 0], seq, x, chain,
            ).wait_send()
            remote(
                part_out.at[layer, pl.ds(0, 7)], part_in.at[layer, pl.ds(0, 7)], rs_send.at[layer],
                rs_recv.at[layer, 0], seq, x, chain,
            ).wait_send()

            @pl.when(seq == 0)
            def _():
                for i in range(1, NY):
                    kv_copy(layer, kv.at[layer], i, seq).wait_send()

            @pl.when(zh == 0)
            def _():
                for i in range(1, NZ):
                    kv_copy(layer, kv.at[layer], NY + i, seq).wait_send()

            @pl.when(jnp.logical_not(out_self(layer)))
            def _():
                out_copy(layer).wait_send()

    for part in range(2):
        for j in range(2):
            @pl.when(jnp.logical_not(is_comm & (x == j)))
            def _():
                x_copy(part, j).wait_send()

    @pl.when(is_chain & (zh == x))
    def _():
        @pl.loop(1, SEQ)
        def _(d):
            ids_copy(d).wait_send()

    @pl.when(is_chain)
    def _():
        @pl.loop(0, 2 * NY)
        def _(k):
            @pl.when(jnp.logical_not(emb_self(k)))
            def _():
                emb_copy(k).wait_send()

    for half in range(2):
        @pl.when(jnp.logical_not(is_chain & (x == 2 + half)))
        def _():
            remote(
                hid.at[0, 0], out_ref.at[:, pl.ds(half * SLICE, SLICE)], out_send.at[0],
                out_recv.at[half], seq, x, tp,
            ).wait_recv()


def rope_constants():
    half = np.arange(HEAD // 2, dtype=np.float64)
    freq = np.float64(ROPE_BASE) ** (-2.0 * half / HEAD)
    freq = np.concatenate([freq, freq])
    coarse = np.arange(SEQ, dtype=np.float64)[:, None] * BLOCK * freq[None]
    fine = np.arange(BLOCK, dtype=np.float64)[:, None] * freq[None]
    pair = lambda angle: np.concatenate([np.cos(angle), np.sin(angle)], axis=1).astype(np.float32)
    return pair(coarse), pair(fine)


def body(token_ids, embed_columns, norm_gain, qkv_weight, out_weight):
    features, vocabulary = embed_columns.shape
    table = embed_columns.reshape(features // 8, 8, vocabulary // HEAD, HEAD).transpose(0, 2, 1, 3)
    rope_a, rope_b = rope_constants()
    bf16, f32 = jnp.bfloat16, jnp.float32
    vmem = pl.BlockSpec(memory_space=pltpu.VMEM)
    dma = pltpu.SemaphoreType.DMA
    states = pl.pallas_call(
        kernel,
        out_shape=jax.ShapeDtypeStruct((BLOCK, 2 * SLICE), bf16),
        in_specs=[vmem, pl.BlockSpec(memory_space=pl.ANY), vmem, vmem, vmem, vmem, vmem],
        out_specs=vmem,
        scratch_shapes=[
            pltpu.VMEM((8, HEAD), jnp.int32),
            pltpu.VMEM((2, ROWS, SLICE), bf16),
            pltpu.VMEM((2, ROWS, 2 * HEAD), bf16),
            pltpu.VMEM((LAYERS, SEQ, ROWS, SLICE), bf16),
            pltpu.VMEM((LAYERS, SEQ, ROWS, 2 * HEAD), bf16),
            pltpu.VMEM(table.shape, bf16),
            pltpu.VMEM(table.shape, bf16),
            pltpu.VMEM((NY, 8, HEAD), jnp.int32),
            pltpu.SMEM((NY, 8, HEAD), jnp.int32),
            pltpu.VMEM((2 * NY, 32, HEAD), bf16),
            pltpu.VMEM((16, 32, HEAD), bf16),
            pltpu.VMEM((LAYERS + 1, GROUP, BLOCK, SLICE), bf16),
            pltpu.VMEM((LAYERS, GROUP, BLOCK, SLICE), bf16),
            pltpu.VMEM((LAYERS, GROUP, BLOCK, SLICE), bf16),
            pltpu.VMEM((LAYERS, BLOCK, 2 * HEAD), bf16),
            pltpu.VMEM((LAYERS, BLOCK, 2 * HEAD), bf16),
            pltpu.VMEM((BLOCK, SLICE), f32),
            pltpu.VMEM((BLOCK, SLICE), f32),
            dma((2, 2)),
            dma((LAYERS, 2)),
            dma((LAYERS, 2)),
            dma((LAYERS, 2, NZ)),
            dma((LAYERS, 2)),
            dma((LAYERS, 2, 2)),
            dma((LAYERS, 2, 2, 3, NZ)),
            dma((LAYERS, 2, 2)),
            dma((LAYERS, 2, 7)),
            dma((LAYERS, 2, 3)),
            dma((LAYERS, 2)),
            dma((SEQ,)),
            dma((NY,)),
            dma,
            dma,
            dma,
            dma,
            dma((2 * NY,)),
            dma((16,)),
            dma((LAYERS,)),
            dma((LAYERS, GROUP)),
            dma((LAYERS,)),
            dma((LAYERS, GROUP)),
            dma((LAYERS, NY + NZ)),
            dma((LAYERS,)),
            dma((LAYERS,)),
            dma((2,)),
        ],
        compiler_params=pltpu.CompilerParams(
            collective_id=0, has_side_effects=True, vmem_limit_bytes=62 * 1024 * 1024
        ),
    )(
        token_ids[None], table, norm_gain, qkv_weight[0], out_weight[0],
        jnp.asarray(rope_a), jnp.asarray(rope_b),
    )
    return states[None]


def solution(mesh):
    placed = (
        P("seq"),
        P(("tp", "seq"), None),
        P("section", None),
        P("section", "seq", "tp"),
        P("section", "seq", "tp"),
    )
    return jax.shard_map(
        body, mesh=mesh, in_specs=placed, out_specs=P("section", "seq", "tp"), check_vma=False
    )
```
